32 devices in a mesh: row: 4 (over y, core), col: 8 (over z, x).
Axes of the slice: x: 2, y: 2, z: 4, core: 2. Of those that a mesh axis runs over, the one named last changes fastest.
Arguments:
- density: float32 [4096, 32768], P('row', 'col'), may hold values from 0 to 1
- design_mask: int32 [32, 256], P('row', 'col'), may hold values 0 or 1
- rebalance: int32 [8192], replicated, may hold values from 0 to 8191, as said below
Outputs:
- balanced: bfloat16 [8192, 128, 128], P(('row', 'col'))
- constraint: float32 [], replicated
The draws below stay inside these ranges and needn't reach their ends.
Inputs may be any that keep to these rules, and one draw needn't show every extreme that they name: `rebalance`: A permutation of the 8192 block numbers. Of the blocks that one device holds, the ones that land among one device's output blocks number exactly 8 or none.
All inputs are finite; a program needn't handle non-finite values. No bound on the sum of `design_mask` on one device may be relied on, other than what follows from the above.
Results may differ from the reference program's by a relative error of at most 0.001.
Values may be sent and summed in bfloat16 or wider, within the bound.
A program may use at most 192 MiB of HBM per device.

```python
import jax
import jax.numpy as jnp
from jax import lax

BS = 128
RADIUS = 16
KR = 8
KC = 32
BLOCKS_DEV = 256
CAP = 8
NX = 4096
NY = 32768
NBLK = 8192
N_ROW = 4
N_COL = 8


def draw_rebalance(key, part):
    device_count = N_ROW * N_COL
    group_count = BLOCKS_DEV // CAP
    base = jax.random.fold_in(key, 11)
    key_order, key_offset, key_source, key_target = jax.random.split(base, 4)
    order = jax.random.permutation(key_order, device_count).astype(jnp.int32)
    inverse = jnp.argsort(order).astype(jnp.int32)
    offsets = jax.random.permutation(key_offset, device_count)[:group_count].astype(jnp.int32)
    source_shuffle = jax.vmap(lambda sub: jax.random.permutation(sub, BLOCKS_DEV))(jax.random.split(key_source, device_count)).astype(jnp.int32)
    target_shuffle = jax.vmap(lambda sub: jax.random.permutation(sub, BLOCKS_DEV))(jax.random.split(key_target, device_count)).astype(jnp.int32)
    positions = jnp.arange(NBLK, dtype=jnp.int32)
    target_dev = positions // BLOCKS_DEV
    target_slot = positions % BLOCKS_DEV
    raw_slot = target_shuffle[target_dev, target_slot]
    group = raw_slot // CAP
    within = raw_slot % CAP
    source_dev = (inverse[target_dev] - offsets[group]) % device_count
    local_block = source_shuffle[source_dev, group * CAP + within]
    source_row = source_dev // N_COL
    source_col = source_dev % N_COL
    block_row = source_row * KR + local_block // KC
    block_col = source_col * KC + local_block % KC
    return (block_row * (KC * N_COL) + block_col).astype(jnp.int32)


def set_ends(entries, own_key, smallest, largest):
    place = [jax.random.randint(jax.random.fold_in(own_key, axis), (), 0, length) for axis, length in enumerate(entries.shape)]
    longest = entries.shape.index(max(entries.shape))
    next_to = place[:longest] + [(place[longest] + 1) % entries.shape[longest]] + place[longest + 1:]
    return entries.at[tuple(place)].set(smallest).at[tuple(next_to)].set(largest)


def levels(key, shape, cuts, smallest, high):
    factor_of = 1.0
    for axis_at, shards_of in cuts:
        heights = jax.random.uniform(jax.random.fold_in(jax.random.fold_in(key, 6), axis_at), (shards_of,), jnp.float32, smallest / len(cuts), high / len(cuts))
        factor_of = factor_of * jnp.repeat(jnp.exp(heights), shape[axis_at] // shards_of).reshape((-1,) + (1,) * (len(shape) - 1 - axis_at))
    return factor_of


def setup_inputs(seed: int = 0) -> dict:
    key_list = jax.random.split(jax.random.key(seed), 4)
    return {
        "density": jnp.clip(1.0 * jax.random.uniform(key_list[0], (NX, NY), jnp.float32) ** levels(key_list[0], (NX, NY), ((0, 4), (1, 8)), -0.2, 0.2), 0.0, 1.0),
        "design_mask": set_ends((jax.random.randint(key_list[1], (NX // BS, NY // BS), 0, 4) < 3).astype(jnp.int32), jax.random.fold_in(key_list[1], 1), 0, 1),
        "rebalance": draw_rebalance(jax.random.fold_in(key_list[3], 71), 0),
    }


SHARPNESS = 32.0
THRESHOLD = 0.5
VOLUME_TARGET = 0.4


def filter_taps():
    sigma = RADIUS / 4.0
    offsets = jnp.arange(2 * RADIUS + 1, dtype=jnp.float32) - RADIUS
    raw_taps = jnp.exp(-offsets * offsets / (2.0 * sigma * sigma))
    return raw_taps / jnp.sum(raw_taps)


def smooth(field, weights, axis):
    length = field.shape[axis]
    widths = [(0, 0), (0, 0)]
    widths[axis] = (RADIUS, RADIUS)
    padded = jnp.pad(field, widths)
    total = jnp.zeros_like(field)
    for offset in range(2 * RADIUS + 1):
        total = total + weights[offset] * lax.slice_in_dim(padded, offset, offset + length, axis=axis)
    return total


def reference(density, design_mask, rebalance):
    weights = filter_taps()
    along_rows = smooth(density, weights, 0)
    filtered = smooth(along_rows, weights, 1)
    cell_mask = jnp.repeat(jnp.repeat(design_mask, BS, 0), BS, 1).astype(jnp.float32)
    lower = jnp.tanh(SHARPNESS * THRESHOLD)
    upper = jnp.tanh(SHARPNESS * (1.0 - THRESHOLD))
    projected = cell_mask * (lower + jnp.tanh(SHARPNESS * (filtered - THRESHOLD))) / (lower + upper)
    constraint = jnp.sum(projected) / (NX * NY) / VOLUME_TARGET - 1.0
    block_rows = NX // BS
    block_cols = NY // BS
    tiles = projected.astype(jnp.bfloat16).reshape(block_rows, BS, block_cols, BS)
    tiles = tiles.transpose(0, 2, 1, 3).reshape(block_rows * block_cols, BS, BS)
    balanced = jnp.take(tiles, rebalance.astype(jnp.int32), axis=0)
    return balanced, constraint
```

```python
import functools

import jax
import jax.numpy as jnp
import numpy as np
from jax import lax
from jax.experimental import pallas as pl
from jax.experimental.pallas import tpu as pltpu
from jax.sharding import PartitionSpec as P

BS = 128
RADIUS = 16
SHARPNESS = 32.0
THRESHOLD = 0.5
VOLUME_TARGET = 0.4
MESH = pl.DeviceIdType.MESH
MIB = 2**20
GROUP = 4
STRIP = BS // RADIUS
SIDES = [(dr, dc) for dr in (-1, 0, 1) for dc in (-1, 0, 1) if dr or dc]


def filter_taps():
    sigma = RADIUS / 4.0
    offsets = np.arange(2 * RADIUS + 1, dtype=np.float64) - RADIUS
    raw_taps = np.exp(-offsets * offsets / (2.0 * sigma * sigma))
    return (raw_taps / raw_taps.sum()).astype(np.float32)


def split(x):
    high = x.astype(jnp.bfloat16)
    return high, (x - high.astype(jnp.float32)).astype(jnp.bfloat16)


def bands():
    taps = filter_taps()
    rows = np.zeros((BS, BS + 2 * RADIUS), np.float32)
    cols = np.zeros((2 * BS, BS), np.float32)
    for out in range(BS):
        for e in range(2 * RADIUS + 1):
            rows[out, out + e] = taps[e]
            source = out + e - RADIUS
            at = source if 0 <= source < BS else BS + source % BS
            cols[at, out] = taps[e]
    return split(jnp.asarray(rows)) + split(jnp.asarray(cols))


def over(x, n):
    if n & (n - 1) == 0:
        return x >> (n.bit_length() - 1), x & (n - 1)
    return lax.div(x, jnp.int32(n)), lax.rem(x, jnp.int32(n))


def project_block(before, own, after, mask, row_high, row_low, col_high, col_low):
    lane = lax.broadcasted_iota(jnp.int32, own.shape, 1)
    side = jnp.where(lane < BS // 2, after, before)
    high, low = split(jnp.concatenate([own, side], axis=1))
    dot = functools.partial(jnp.dot, preferred_element_type=jnp.float32)
    along = dot(high, col_high[...]) + (dot(low, col_high[...]) + dot(high, col_low[...]))
    high, low = split(along)
    filtered = dot(row_high[...], high) + (dot(row_high[...], low) + dot(row_low[...], high))
    lower = float(np.tanh(np.float32(SHARPNESS * THRESHOLD)))
    upper = float(np.tanh(np.float32(SHARPNESS * (1.0 - THRESHOLD))))
    return (lower + jnp.tanh(SHARPNESS * (filtered - THRESHOLD))) * (mask.astype(jnp.float32) / (lower + upper))


def upto_lane(x):
    lane = lax.broadcasted_iota(jnp.int32, x.shape, 1)
    step = 1
    while step < x.shape[1]:
        x = x + jnp.where(lane >= step, pltpu.roll(x, step, 1), 0)
        step *= 2
    return x


def locate(wanted, mask_rows, mask_cols, col_count):
    block_row, block_col = over(wanted, mask_cols * col_count)
    row_dev, row_in = over(block_row, mask_rows)
    col_dev, col_in = over(block_col, mask_cols)
    return row_dev * col_count + col_dev, row_in * mask_cols + col_in


def pick(chosen, rank, values, capacity):
    lane = lax.broadcasted_iota(jnp.int32, chosen.shape, 1)
    out = jnp.zeros(chosen.shape, jnp.int32)
    for k in range(capacity):
        found = jnp.sum(jnp.where(chosen & (rank == k + 1), values, 0), axis=1, keepdims=True)
        out = jnp.where(lane == k, found, out)
    return out


def send_order(wanted, me, per, mask_rows, mask_cols, col_count, capacity):
    source, local = locate(wanted, mask_rows, mask_cols, col_count)
    mine = source == me
    rank = upto_lane(mine.astype(jnp.int32))
    count = jnp.broadcast_to(rank[:, BS - 1 :], rank.shape)
    _, part = over(lax.broadcasted_iota(jnp.int32, rank.shape, 0), per)
    for j in range(1, per):
        rank = rank + jnp.where(part >= j, pltpu.roll(count, j, 0), 0)
    return pick(mine, rank, local, capacity)


def landing(wanted, devices, mask_rows, mask_cols, col_count, capacity):
    row = lax.broadcasted_iota(jnp.int32, (devices, BS), 0)
    lane = lax.broadcasted_iota(jnp.int32, (devices, BS), 1)
    before = jnp.zeros((devices, 1), jnp.int32)
    out = jnp.zeros((devices, BS), jnp.int32)
    for j in range(wanted.shape[0]):
        source, _ = locate(jnp.broadcast_to(wanted[j : j + 1], (devices, BS)), mask_rows, mask_cols, col_count)
        here = source == row
        rank = upto_lane(here.astype(jnp.int32)) + before
        before = rank[:, BS - 1 :]
        out = out + pick(here, rank, lane + j * BS, capacity)
    return out


def exchange_kernel(
    sizes, mask, density, rebalance, rh_in, rl_in, ch_in, cl_in,
    arrived, volume, slots, padded, outgoing, total, sums, wanted, order, table, rh, rl, ch, cl,
    strip_out, strip_in, rows_in, load_sem, small_sem, side_send, side_recv, send_sem, recv_sem, sum_send, sum_recv,
):
    row_count, col_count = sizes
    devices, capacity = outgoing.shape[:2]
    group = min(GROUP, capacity)
    mask_rows, mask_cols = mask.shape
    bands_of_rows, _, width = density.shape
    height = bands_of_rows * RADIUS
    last = bands_of_rows + 1
    per = wanted.shape[0] // devices
    row, col = lax.axis_index("row"), lax.axis_index("col")
    me = row * col_count + col
    half, quarter = col_count // 2, col_count // 4
    near = quarter * row_count

    def place_of(device):
        return (device // col_count, device % col_count)

    def target(turn):
        early = 1 - turn // (3 * near)
        is_beside = early * (turn % 3 // 2)
        is_across = early - is_beside
        across, beside, close = turn // 3 * 2 + turn % 3, turn // 3, (turn + 1) % near
        far_col = ((col // half + 1) % 2) * half + (col + across) % half
        beside_col = col // half * half + ((col // quarter + 1) % 2) * quarter + (col + beside) % quarter
        close_col = col // quarter * quarter + (col + close) % quarter
        to_col = is_across * far_col + is_beside * beside_col + (1 - early) * close_col
        step = is_across * (across // half) + is_beside * (beside // quarter) + (1 - early) * (close // quarter)
        return (row + step) % row_count * col_count + to_col

    def send(device, k):
        part = pl.ds(k, group)
        return pltpu.make_async_remote_copy(
            src_ref=outgoing.at[device, part], dst_ref=arrived.at[me, part], send_sem=send_sem.at[device],
            recv_sem=recv_sem.at[me], device_id=place_of(device), device_id_type=MESH,
        )

    def receive(device):
        return pltpu.make_async_remote_copy(
            src_ref=outgoing.at[device], dst_ref=arrived.at[device], send_sem=send_sem.at[device],
            recv_sem=recv_sem.at[device], device_id=place_of(device), device_id_type=MESH,
        )

    def send_sum(device):
        return pltpu.make_async_remote_copy(
            src_ref=sums.at[me], dst_ref=sums.at[me], send_sem=sum_send.at[device],
            recv_sem=sum_recv.at[me], device_id=place_of(device), device_id_type=MESH,
        )

    def receive_sum(device):
        return pltpu.make_async_remote_copy(
            src_ref=sums.at[me], dst_ref=sums.at[device], send_sem=sum_send.at[device],
            recv_sem=sum_recv.at[device], device_id=place_of(device), device_id_type=MESH,
        )

    def side_copy(dr, dc):
        at = SIDES.index((dr, dc))
        band, goal_band = {-1: 0, 1: bands_of_rows - 1}, {-1: last, 1: 0}
        cols = {-1: pl.ds(0, BS), 1: pl.ds(width - BS, BS)}
        goal_col = {-1: mask_cols + 1, 1: 0}
        if dr == 0:
            source, goal = strip_out.at[(dc + 1) // 2], strip_in.at[(dc + 1) // 2]
        elif dc == 0:
            source, goal = density.at[band[dr]], rows_in.at[(dr + 1) // 2]
        else:
            source, goal = density.at[band[dr], :, cols[dc]], padded.at[goal_col[dc], goal_band[dr]]
        return pltpu.make_async_remote_copy(
            src_ref=source, dst_ref=goal, send_sem=side_send.at[at], recv_sem=side_recv.at[at],
            device_id=(row + dr, col + dc), device_id_type=MESH,
        )

    def there(dr, dc):
        return (row + dr >= 0) & (row + dr < row_count) & (col + dc >= 0) & (col + dc < col_count)

    barrier = pltpu.get_barrier_semaphore()

    @pl.loop(1, devices)
    def _(o):
        pl.semaphore_signal(barrier, inc=1, device_id=place_of((me + o) % devices), device_id_type=MESH)

    small = [
        pltpu.make_async_copy(source, goal, small_sem.at[i])
        for i, (source, goal) in enumerate(
            [(rebalance, wanted), (rh_in, rh), (rl_in, rl), (ch_in, ch), (cl_in, cl)]
        )
    ]

    def load(c, sem):
        source = density.at[:, :, pl.ds(pl.multiple_of(c * BS, BS), BS)]
        return pltpu.make_async_copy(source, padded.at[c + 1, pl.ds(1, bands_of_rows)], load_sem.at[sem])

    edges = [load(0, 0), load(mask_cols - 1, 1)]
    small[0].start()
    for copy in edges + small[1:]:
        copy.start()

    @pl.loop(1, mask_cols - 1)
    def _(c):
        load(c, 2).start()

    total[...] = jnp.zeros_like(total)

    @pl.when(row == 0)
    def _():
        padded[:, 0] = jnp.zeros((mask_cols + 2, RADIUS, BS), jnp.float32)

    @pl.when(row == row_count - 1)
    def _():
        padded[:, last] = jnp.zeros((mask_cols + 2, RADIUS, BS), jnp.float32)

    @pl.when(col == 0)
    def _():
        padded[0] = jnp.zeros(padded.shape[1:], jnp.float32)

    @pl.when(col == col_count - 1)
    def _():
        padded[mask_cols + 1] = jnp.zeros(padded.shape[1:], jnp.float32)

    piece = height // STRIP
    parts = piece // RADIUS
    spot, _ = over(lax.broadcasted_iota(jnp.int32, (piece, BS), 1), RADIUS)
    for side, copy in enumerate(edges):
        copy.wait()
        strip = jnp.zeros((piece, BS), jnp.float32)
        for p in range(STRIP):
            edge = padded[1 + side * (mask_cols - 1), pl.ds(1 + p * parts, parts)].reshape(piece, BS)
            strip = jnp.where(spot == p, pltpu.roll(edge, (p * RADIUS + side * RADIUS) % BS, 1), strip)
        strip_out[side] = strip

    small[0].wait()
    order[...] = send_order(wanted[...], me, per, mask_rows, mask_cols, col_count, capacity)
    pl.semaphore_wait(barrier, devices - 1)
    for dr, dc in SIDES:

        @pl.when(there(dr, dc))
        def _():
            side_copy(dr, dc).start()

    to_scalars = pltpu.make_async_copy(order, table, small_sem.at[5])
    to_scalars.start()
    slots[...] = landing(
        wanted[pl.ds(me * per, per), :], devices, mask_rows, mask_cols, col_count, capacity
    )
    for dr, dc in SIDES:

        @pl.when(there(-dr, -dc))
        def _():
            side_copy(dr, dc).wait_recv()
            if dr == 0:
                strip = strip_in[(dc + 1) // 2]
                for p in range(STRIP):
                    shift = (BS - p * RADIUS - (dc + 1) // 2 * RADIUS) % BS
                    moved = pltpu.roll(strip, shift, 1).reshape(parts, RADIUS, BS)
                    padded[0 if dc == 1 else mask_cols + 1, pl.ds(1 + p * parts, parts)] = moved
            elif dc == 0:
                for c in range(mask_cols):
                    padded[c + 1, 0 if dr == 1 else last] = rows_in[(dr + 1) // 2, :, pl.ds(c * BS, BS)]

        @pl.when(there(dr, dc))
        def _():
            side_copy(dr, dc).wait_send()

    middle = padded.at[pl.ds(2, mask_cols - 2), pl.ds(1, bands_of_rows)]
    pltpu.make_async_copy(middle, middle, load_sem.at[2]).wait()
    for copy in small[1:]:
        copy.wait()
    to_scalars.wait()

    @pl.loop(0, devices * capacity)
    def _(n):
        turn, k = n // capacity, n % capacity
        device = target(turn)
        local = table[device * per, k]
        for j in range(1, per):
            local = local + table[device * per + j, k]
        r, c = over(local, mask_cols)
        deep = BS // RADIUS
        before, own, after = (
            jnp.concatenate([padded[c + i, r * deep + j] for j in range(deep + 2)], axis=0) for i in range(3)
        )
        cells = project_block(before, own, after, mask[r, c], rh, rl, ch, cl)
        total[...] += cells
        outgoing[device, k] = cells.astype(jnp.bfloat16)

        @pl.when((n % group == 0) & (n > 0) & (n <= (devices - 1) * capacity))
        def _():
            send(target((n - 1) // capacity), (n - 1) % capacity // group * group).start()

    sums[me] = jnp.sum(total[...].reshape(BS // 8, 8, BS), axis=0)
    arrived[me] = outgoing[me]

    @pl.loop(1, devices)
    def _(o):
        send_sum((me + o) % devices).start()

    @pl.loop(1, devices)
    def _(o):
        other = (me + o) % devices
        send_sum(other).wait_send()
        receive_sum(other).wait_recv()

    volume[...] = jnp.sum(sums[...], axis=0)

    @pl.loop(1, devices)
    def _(o):
        other = (me + o) % devices
        receive(other).wait_send()
        receive(other).wait_recv()


def exchange(mask, density, rebalance, sizes):
    devices = sizes[0] * sizes[1]
    capacity = mask.size // devices
    height, width = density.shape
    in_hbm = pl.BlockSpec(memory_space=pltpu.HBM)
    whole = pl.BlockSpec(memory_space=pltpu.VMEM)
    scalar = pl.BlockSpec(memory_space=pltpu.SMEM)
    cells = devices * capacity * BS * BS
    band = bands()
    wanted = rebalance.reshape(-1, BS)
    table = pltpu.VMEM(wanted.shape, jnp.int32)
    strips = pltpu.VMEM((2, height // STRIP, BS), jnp.float32)
    return pl.pallas_call(
        functools.partial(exchange_kernel, sizes),
        out_shape=(
            jax.ShapeDtypeStruct((devices, capacity, BS, BS), jnp.bfloat16),
            jax.ShapeDtypeStruct((8, BS), jnp.float32),
            jax.ShapeDtypeStruct((devices, BS), jnp.int32),
        ),
        in_specs=[scalar] + [in_hbm] * 6,
        out_specs=(whole, whole, whole),
        scratch_shapes=[
            pltpu.VMEM((width // BS + 2, height // RADIUS + 2, RADIUS, BS), jnp.float32),
            pltpu.VMEM((devices, capacity, BS, BS), jnp.bfloat16),
            pltpu.VMEM((BS, BS), jnp.float32),
            pltpu.VMEM((devices, 8, BS), jnp.float32),
            table,
            table,
            pltpu.SMEM(wanted.shape, jnp.int32),
        ]
        + [pltpu.VMEM(x.shape, x.dtype) for x in band]
        + [
            strips,
            strips,
            pltpu.VMEM((2, RADIUS, width), jnp.float32),
            pltpu.SemaphoreType.DMA((3,)),
            pltpu.SemaphoreType.DMA((6,)),
            pltpu.SemaphoreType.DMA((len(SIDES),)),
            pltpu.SemaphoreType.DMA((len(SIDES),)),
        ]
        + [pltpu.SemaphoreType.DMA((devices,))] * 4,
        compiler_params=pltpu.CompilerParams(vmem_limit_bytes=40 * MIB, collective_id=0, has_side_effects=True),
        cost_estimate=pl.CostEstimate(flops=cells * 2000, bytes_accessed=density.size * 4, transcendentals=cells),
        name="exchange",
    )(mask, density.reshape(height // RADIUS, RADIUS, width), wanted, *band)


def place_kernel(cells, slots, arrived, volume, out, constraint, store_sem):
    devices, capacity = arrived.shape[:2]

    @pl.loop(0, devices)
    def _(d):
        for k in range(capacity):
            pltpu.make_async_copy(arrived.at[d, k], out.at[slots[d, k]], store_sem).start()

    mean = jnp.sum(volume[...], keepdims=True) / cells
    constraint[...] = mean / VOLUME_TARGET - 1.0
    landed = out.at[pl.ds(0, devices * capacity)]
    pltpu.make_async_copy(landed, landed, store_sem).wait()


def place(slots, arrived, volume, cells):
    count = arrived.shape[0] * arrived.shape[1]
    whole = pl.BlockSpec(memory_space=pltpu.VMEM)
    return pl.pallas_call(
        functools.partial(place_kernel, cells),
        out_shape=(
            jax.ShapeDtypeStruct((count, BS, BS), jnp.bfloat16),
            jax.ShapeDtypeStruct((1, 1), jnp.float32),
        ),
        in_specs=[pl.BlockSpec(memory_space=pltpu.SMEM), whole, whole],
        out_specs=(pl.BlockSpec(memory_space=pltpu.HBM), whole),
        scratch_shapes=[pltpu.SemaphoreType.DMA],
        compiler_params=pltpu.CompilerParams(vmem_limit_bytes=8 * MIB),
        cost_estimate=pl.CostEstimate(flops=0, bytes_accessed=2 * arrived.size * 2, transcendentals=0),
        name="place",
    )(slots, arrived, volume)


def per_device(density, design_mask, rebalance):
    sizes = (lax.axis_size("row"), lax.axis_size("col"))
    arrived, volume, slots = exchange(design_mask, density, rebalance, sizes)
    balanced, constraint = place(slots, arrived, volume, float(density.size * sizes[0] * sizes[1]))
    return balanced, constraint[0, 0]


def solution(mesh):
    return jax.shard_map(
        per_device,
        mesh=mesh,
        in_specs=(P("row", "col"), P("row", "col"), P()),
        out_specs=(P(("row", "col"), None, None), P()),
        check_vma=False,
    )
```

```python
import functools

import jax
import jax.numpy as jnp
import numpy as np
from jax import lax
from jax.experimental import pallas as pl
from jax.experimental.pallas import tpu as pltpu
from jax.sharding import PartitionSpec as P

BS = 128
RADIUS = 16
SHARPNESS = 32.0
THRESHOLD = 0.5
VOLUME_TARGET = 0.4
MESH = pl.DeviceIdType.MESH
MIB = 2**20
GROUP = 2
STRIP = BS // RADIUS
SIDES = [(dr, dc) for dr in (-1, 0, 1) for dc in (-1, 0, 1) if dr or dc]


def filter_taps():
    sigma = RADIUS / 4.0
    offsets = np.arange(2 * RADIUS + 1, dtype=np.float64) - RADIUS
    raw_taps = np.exp(-offsets * offsets / (2.0 * sigma * sigma))
    return (raw_taps / raw_taps.sum()).astype(np.float32)


def split(x):
    high = x.astype(jnp.bfloat16)
    return high, (x - high.astype(jnp.float32)).astype(jnp.bfloat16)


def band(distance):
    taps = filter_taps()
    weight = jnp.zeros(distance.shape, jnp.float32)
    for far in range(RADIUS + 1):
        weight = jnp.where(distance == far, float(taps[RADIUS + far]), weight)
    return split(weight)


def col_bands():
    source = lax.broadcasted_iota(jnp.int32, (2 * BS, BS), 0)
    source = jnp.where(source < BS + BS // 2, source, source - 2 * BS)
    return band(jnp.abs(source - lax.broadcasted_iota(jnp.int32, source.shape, 1)))


def row_bands():
    source = lax.broadcasted_iota(jnp.int32, (BS, BS + 2 * RADIUS), 1) - RADIUS
    return band(jnp.abs(source - lax.broadcasted_iota(jnp.int32, source.shape, 0)))


def over(x, n):
    if n & (n - 1) == 0:
        return x >> (n.bit_length() - 1), x & (n - 1)
    return lax.div(x, jnp.int32(n)), lax.rem(x, jnp.int32(n))


def project_block(before, own, after, mask, row_high, row_low, col_high, col_low):
    lane = lax.broadcasted_iota(jnp.int32, own.shape, 1)
    side = jnp.where(lane < BS // 2, after, before)
    high, low = split(jnp.concatenate([own, side], axis=1))
    dot = functools.partial(jnp.dot, preferred_element_type=jnp.float32)
    along = dot(high, col_high[...]) + (dot(low, col_high[...]) + dot(high, col_low[...]))
    high, low = split(along)
    filtered = dot(row_high[...], high) + (dot(row_high[...], low) + dot(row_low[...], high))
    lower = float(np.tanh(np.float32(SHARPNESS * THRESHOLD)))
    upper = float(np.tanh(np.float32(SHARPNESS * (1.0 - THRESHOLD))))
    return (lower + jnp.tanh(SHARPNESS * (filtered - THRESHOLD))) * (mask.astype(jnp.float32) / (lower + upper))


def upto_lane(x):
    lane = lax.broadcasted_iota(jnp.int32, x.shape, 1)
    step = 1
    while step < x.shape[1]:
        x = x + jnp.where(lane >= step, pltpu.roll(x, step, 1), 0)
        step *= 2
    return x


def locate(wanted, mask_rows, mask_cols, col_count):
    block_row, block_col = over(wanted, mask_cols * col_count)
    row_dev, row_in = over(block_row, mask_rows)
    col_dev, col_in = over(block_col, mask_cols)
    return row_dev * col_count + col_dev, row_in * mask_cols + col_in


def pick(chosen, rank, values, capacity):
    lane = lax.broadcasted_iota(jnp.int32, chosen.shape, 1)
    out = jnp.zeros(chosen.shape, jnp.int32)
    for k in range(capacity):
        found = jnp.sum(jnp.where(chosen & (rank == k + 1), values, 0), axis=1, keepdims=True)
        out = jnp.where(lane == k, found, out)
    return out


def send_order(wanted, me, per, mask_rows, mask_cols, col_count, capacity):
    source, local = locate(wanted, mask_rows, mask_cols, col_count)
    mine = source == me
    rank = upto_lane(mine.astype(jnp.int32))
    count = jnp.broadcast_to(rank[:, BS - 1 :], rank.shape)
    _, part = over(lax.broadcasted_iota(jnp.int32, rank.shape, 0), per)
    for j in range(1, per):
        rank = rank + jnp.where(part >= j, pltpu.roll(count, j, 0), 0)
    return pick(mine, rank, local, capacity)


def landing(wanted, devices, mask_rows, mask_cols, col_count, capacity):
    row = lax.broadcasted_iota(jnp.int32, (devices, BS), 0)
    lane = lax.broadcasted_iota(jnp.int32, (devices, BS), 1)
    before = jnp.zeros((devices, 1), jnp.int32)
    out = jnp.zeros((devices, BS), jnp.int32)
    for j in range(wanted.shape[0]):
        source, _ = locate(jnp.broadcast_to(wanted[j : j + 1], (devices, BS)), mask_rows, mask_cols, col_count)
        here = source == row
        rank = upto_lane(here.astype(jnp.int32)) + before
        before = rank[:, BS - 1 :]
        out = out + pick(here, rank, lane + j * BS, capacity)
    return out


def exchange_kernel(
    sizes, mask_rows, mask_cols, density, known,
    arrived, volume, slots, padded, outgoing, total, sums, order, table, rh, rl, ch, cl,
    strip_out, strip_in, rows_out, rows_in, load_sem, side_send, side_recv, send_sem, recv_sem, sum_send, sum_recv,
):
    row_count, col_count = sizes
    devices, capacity = outgoing.shape[:2]
    group = min(GROUP, capacity)
    wanted = known[: known.shape[0] - mask_rows]
    bands_of_rows, _, width = density.shape
    height = bands_of_rows * RADIUS
    last = bands_of_rows + 1
    per = wanted.shape[0] // devices
    row, col = lax.axis_index("row"), lax.axis_index("col")
    me = row * col_count + col
    half, quarter = col_count // 2, col_count // 4
    near = quarter * row_count

    def place_of(device):
        return (device // col_count, device % col_count)

    def target(turn):
        early = 1 - turn // (3 * near)
        is_beside = early * (turn % 3 // 2)
        is_across = early - is_beside
        across, beside, close = turn // 3 * 2 + turn % 3, turn // 3, (turn + 1) % near
        far_col = ((col // half + 1) % 2) * half + (col + across) % half
        beside_col = col // half * half + ((col // quarter + 1) % 2) * quarter + (col + beside) % quarter
        close_col = col // quarter * quarter + (col + close) % quarter
        to_col = is_across * far_col + is_beside * beside_col + (1 - early) * close_col
        step = is_across * (across // half) + is_beside * (beside // quarter) + (1 - early) * (close // quarter)
        return (row + step) % row_count * col_count + to_col

    def send(device, k):
        part = pl.ds(k, group)
        return pltpu.make_async_remote_copy(
            src_ref=outgoing.at[device, part], dst_ref=arrived.at[me, part], send_sem=send_sem.at[device],
            recv_sem=recv_sem.at[me], device_id=place_of(device), device_id_type=MESH,
        )

    def receive(device):
        return pltpu.make_async_remote_copy(
            src_ref=outgoing.at[device], dst_ref=arrived.at[device], send_sem=send_sem.at[device],
            recv_sem=recv_sem.at[device], device_id=place_of(device), device_id_type=MESH,
        )

    def send_sum(device):
        return pltpu.make_async_remote_copy(
            src_ref=sums.at[me], dst_ref=sums.at[me], send_sem=sum_send.at[device],
            recv_sem=sum_recv.at[me], device_id=place_of(device), device_id_type=MESH,
        )

    def receive_sum(device):
        return pltpu.make_async_remote_copy(
            src_ref=sums.at[me], dst_ref=sums.at[device], send_sem=sum_send.at[device],
            recv_sem=sum_recv.at[device], device_id=place_of(device), device_id_type=MESH,
        )

    def side_copy(dr, dc):
        at = SIDES.index((dr, dc))
        edge, goal_band = {-1: 0, 1: bands_of_rows - 1}, {-1: last, 1: 0}
        cols = {-1: pl.ds(0, BS), 1: pl.ds(width - BS, BS)}
        goal_col = {-1: mask_cols + 1, 1: 0}
        if dr == 0:
            source, goal = strip_out.at[(dc + 1) // 2], strip_in.at[(dc + 1) // 2]
        elif dc == 0:
            source, goal = rows_out.at[(dr + 1) // 2], rows_in.at[(dr + 1) // 2]
        else:
            source, goal = density.at[edge[dr], :, cols[dc]], padded.at[goal_col[dc], goal_band[dr]]
        return pltpu.make_async_remote_copy(
            src_ref=source, dst_ref=goal, send_sem=side_send.at[at], recv_sem=side_recv.at[at],
            device_id=(row + dr, col + dc), device_id_type=MESH,
        )

    def there(dr, dc):
        return (row + dr >= 0) & (row + dr < row_count) & (col + dc >= 0) & (col + dc < col_count)

    barrier = pltpu.get_barrier_semaphore()

    @pl.loop(1, devices)
    def _(o):
        pl.semaphore_signal(barrier, inc=1, device_id=place_of((me + o) % devices), device_id_type=MESH)

    def load(c, sem):
        source = density.at[:, :, pl.ds(pl.multiple_of(c * BS, BS), BS)]
        return pltpu.make_async_copy(source, padded.at[c + 1, pl.ds(1, bands_of_rows)], load_sem.at[sem])

    edges = [load(0, 0), load(mask_cols - 1, 1)]
    rows = [
        pltpu.make_async_copy(density.at[at], rows_out.at[side], load_sem.at[3 + side])
        for side, at in enumerate((0, bands_of_rows - 1))
    ]
    for copy in edges + rows:
        copy.start()

    @pl.loop(1, mask_cols - 1)
    def _(c):
        load(c, 2).start()

    total[...] = jnp.zeros_like(total)

    @pl.when(row == 0)
    def _():
        padded[:, 0] = jnp.zeros((mask_cols + 2, RADIUS, BS), jnp.float32)

    @pl.when(row == row_count - 1)
    def _():
        padded[:, last] = jnp.zeros((mask_cols + 2, RADIUS, BS), jnp.float32)

    @pl.when(col == 0)
    def _():
        padded[0] = jnp.zeros(padded.shape[1:], jnp.float32)

    @pl.when(col == col_count - 1)
    def _():
        padded[mask_cols + 1] = jnp.zeros(padded.shape[1:], jnp.float32)

    piece = height // STRIP
    parts = piece // RADIUS
    spot, _ = over(lax.broadcasted_iota(jnp.int32, (piece, BS), 1), RADIUS)
    for side, copy in enumerate(edges):
        copy.wait()
        strip = jnp.zeros((piece, BS), jnp.float32)
        for p in range(STRIP):
            edge = padded[1 + side * (mask_cols - 1), pl.ds(1 + p * parts, parts)].reshape(piece, BS)
            strip = jnp.where(spot == p, pltpu.roll(edge, (p * RADIUS + side * RADIUS) % BS, 1), strip)
        strip_out[side] = strip

    order[0 : wanted.shape[0]] = send_order(wanted, me, per, mask_rows, mask_cols, col_count, capacity)
    order[wanted.shape[0] :] = known[wanted.shape[0] :]
    to_scalars = pltpu.make_async_copy(order, table, load_sem.at[5])
    to_scalars.start()
    for copy in rows:
        copy.wait()
    pl.semaphore_wait(barrier, devices - 1)
    for dr, dc in SIDES:

        @pl.when(there(dr, dc))
        def _():
            side_copy(dr, dc).start()

    rh[...], rl[...] = row_bands()
    ch[...], cl[...] = col_bands()
    slots[...] = landing(
        known[pl.ds(me * per, per), :], devices, mask_rows, mask_cols, col_count, capacity
    )
    for dr, dc in SIDES:

        @pl.when(there(-dr, -dc))
        def _():
            side_copy(dr, dc).wait_recv()
            if dr == 0:
                strip = strip_in[(dc + 1) // 2]
                for p in range(STRIP):
                    shift = (BS - p * RADIUS - (dc + 1) // 2 * RADIUS) % BS
                    moved = pltpu.roll(strip, shift, 1).reshape(parts, RADIUS, BS)
                    padded[0 if dc == 1 else mask_cols + 1, pl.ds(1 + p * parts, parts)] = moved
            elif dc == 0:
                for c in range(mask_cols):
                    padded[c + 1, 0 if dr == 1 else last] = rows_in[(dr + 1) // 2, :, pl.ds(c * BS, BS)]

        @pl.when(there(dr, dc))
        def _():
            side_copy(dr, dc).wait_send()

    middle = padded.at[pl.ds(2, mask_cols - 2), pl.ds(1, bands_of_rows)]
    pltpu.make_async_copy(middle, middle, load_sem.at[2]).wait()
    to_scalars.wait()

    def block(device, k):
        local = table[device * per, k]
        for j in range(1, per):
            local = local + table[device * per + j, k]
        r, c = over(local, mask_cols)
        deep = BS // RADIUS
        before, own, after = (
            jnp.concatenate([padded[c + i, r * deep + j] for j in range(deep + 2)], axis=0) for i in range(3)
        )
        cells = project_block(before, own, after, table[wanted.shape[0] + r, c], rh, rl, ch, cl)
        outgoing[device, k] = cells.astype(jnp.bfloat16)
        return cells

    def turns(turn, before):
        device = target(turn)

        @pl.loop(0, capacity // group)
        def _(p):
            total[...] += sum(block(device, p * group + k) for k in range(group))

            @pl.when(p > 0)
            def _():
                @pl.when(turn < devices - 1)
                def _():
                    send(device, (p - 1) * group).start()

            @pl.when(p == 0)
            def _():
                @pl.when(turn > 0)
                def _():
                    send(before, capacity - group).start()

        return device

    lax.fori_loop(0, devices, turns, me)
    sums[me] = jnp.sum(total[...].reshape(BS // 8, 8, BS), axis=0)
    arrived[me] = outgoing[me]

    @pl.loop(1, devices)
    def _(o):
        send_sum((me + o) % devices).start()

    @pl.loop(1, devices)
    def _(o):
        other = (me + o) % devices
        send_sum(other).wait_send()
        receive_sum(other).wait_recv()

    volume[...] = jnp.sum(sums[...], axis=0)

    @pl.loop(1, devices)
    def _(o):
        other = (me + o) % devices
        receive(other).wait_send()
        receive(other).wait_recv()


def exchange(mask, density, rebalance, sizes):
    devices = sizes[0] * sizes[1]
    capacity = mask.size // devices
    height, width = density.shape
    in_hbm = pl.BlockSpec(memory_space=pltpu.HBM)
    whole = pl.BlockSpec(memory_space=pltpu.VMEM)
    cells = devices * capacity * BS * BS
    known = jnp.concatenate([rebalance.reshape(-1, BS), jnp.pad(mask, ((0, 0), (0, BS - mask.shape[1])))])
    strips = pltpu.VMEM((2, height // STRIP, BS), jnp.float32)
    rows = pltpu.VMEM((2, RADIUS, width), jnp.float32)
    row_band = pltpu.VMEM((BS, BS + 2 * RADIUS), jnp.bfloat16)
    col_band = pltpu.VMEM((2 * BS, BS), jnp.bfloat16)
    return pl.pallas_call(
        functools.partial(exchange_kernel, sizes, *mask.shape),
        out_shape=(
            jax.ShapeDtypeStruct((devices, capacity, BS, BS), jnp.bfloat16),
            jax.ShapeDtypeStruct((8, BS), jnp.float32),
            jax.ShapeDtypeStruct((devices, BS), jnp.int32),
        ),
        in_specs=[in_hbm, whole],
        out_specs=(whole, whole, whole),
        scratch_shapes=[
            pltpu.VMEM((width // BS + 2, height // RADIUS + 2, RADIUS, BS), jnp.float32),
            pltpu.VMEM((devices, capacity, BS, BS), jnp.bfloat16),
            pltpu.VMEM((BS, BS), jnp.float32),
            pltpu.VMEM((devices, 8, BS), jnp.float32),
            pltpu.VMEM(known.shape, jnp.int32),
            pltpu.SMEM(known.shape, jnp.int32),
            row_band,
            row_band,
            col_band,
            col_band,
            strips,
            strips,
            rows,
            rows,
            pltpu.SemaphoreType.DMA((6,)),
            pltpu.SemaphoreType.DMA((len(SIDES),)),
            pltpu.SemaphoreType.DMA((len(SIDES),)),
        ]
        + [pltpu.SemaphoreType.DMA((devices,))] * 4,
        compiler_params=pltpu.CompilerParams(vmem_limit_bytes=40 * MIB, collective_id=0, has_side_effects=True),
        cost_estimate=pl.CostEstimate(flops=cells * 2000, bytes_accessed=density.size * 4, transcendentals=cells),
        name="exchange",
    )(density.reshape(height // RADIUS, RADIUS, width), known)


def place_kernel(cells, slots, arrived, volume, out, constraint, store_sem):
    devices, capacity = arrived.shape[:2]

    @pl.loop(0, devices)
    def _(d):
        for k in range(capacity):
            pltpu.make_async_copy(arrived.at[d, k], out.at[slots[d, k]], store_sem).start()

    mean = jnp.sum(volume[...], keepdims=True) / cells
    constraint[...] = mean / VOLUME_TARGET - 1.0
    landed = out.at[pl.ds(0, devices * capacity)]
    pltpu.make_async_copy(landed, landed, store_sem).wait()


def place(slots, arrived, volume, cells):
    count = arrived.shape[0] * arrived.shape[1]
    whole = pl.BlockSpec(memory_space=pltpu.VMEM)
    return pl.pallas_call(
        functools.partial(place_kernel, cells),
        out_shape=(
            jax.ShapeDtypeStruct((count, BS, BS), jnp.bfloat16),
            jax.ShapeDtypeStruct((1, 1), jnp.float32),
        ),
        in_specs=[pl.BlockSpec(memory_space=pltpu.SMEM), whole, whole],
        out_specs=(pl.BlockSpec(memory_space=pltpu.HBM), whole),
        scratch_shapes=[pltpu.SemaphoreType.DMA],
        compiler_params=pltpu.CompilerParams(vmem_limit_bytes=8 * MIB),
        cost_estimate=pl.CostEstimate(flops=0, bytes_accessed=2 * arrived.size * 2, transcendentals=0),
        name="place",
    )(slots, arrived, volume)


def per_device(density, design_mask, rebalance):
    sizes = (lax.axis_size("row"), lax.axis_size("col"))
    arrived, volume, slots = exchange(design_mask, density, rebalance, sizes)
    balanced, constraint = place(slots, arrived, volume, float(density.size * sizes[0] * sizes[1]))
    return balanced, constraint[0, 0]


def solution(mesh):
    return jax.shard_map(
        per_device,
        mesh=mesh,
        in_specs=(P("row", "col"), P("row", "col"), P()),
        out_specs=(P(("row", "col"), None, None), P()),
        check_vma=False,
    )
```

```python
import functools

import jax
import jax.numpy as jnp
import numpy as np
from jax import lax
from jax.experimental import pallas as pl
from jax.experimental.pallas import tpu as pltpu
from jax.sharding import PartitionSpec as P

BS = 128
RADIUS = 16
SHARPNESS = 32.0
THRESHOLD = 0.5
VOLUME_TARGET = 0.4
MESH = pl.DeviceIdType.MESH
MIB = 2**20
GROUP = 2
SLACK = 2
STRIP = BS // RADIUS
SIDES = [(dr, dc) for dr in (-1, 0, 1) for dc in (-1, 0, 1) if dr or dc]


def filter_taps():
    sigma = RADIUS / 4.0
    offsets = np.arange(2 * RADIUS + 1, dtype=np.float64) - RADIUS
    raw_taps = np.exp(-offsets * offsets / (2.0 * sigma * sigma))
    return (raw_taps / raw_taps.sum()).astype(np.float32)


def split(x):
    high = x.astype(jnp.bfloat16)
    return high, (x - high.astype(jnp.float32)).astype(jnp.bfloat16)


def band(distance):
    taps = filter_taps()
    weight = jnp.zeros(distance.shape, jnp.float32)
    for far in range(RADIUS + 1):
        weight = jnp.where(distance == far, float(taps[RADIUS + far]), weight)
    return split(weight)


def col_bands():
    source = lax.broadcasted_iota(jnp.int32, (2 * BS, BS), 0)
    source = jnp.where(source < BS + BS // 2, source, source - 2 * BS)
    return band(jnp.abs(source - lax.broadcasted_iota(jnp.int32, source.shape, 1)))


def row_bands():
    source = lax.broadcasted_iota(jnp.int32, (BS, BS + 2 * RADIUS), 1) - RADIUS
    return band(jnp.abs(source - lax.broadcasted_iota(jnp.int32, source.shape, 0)))


def over(x, n):
    if n & (n - 1) == 0:
        return x >> (n.bit_length() - 1), x & (n - 1)
    return lax.div(x, jnp.int32(n)), lax.rem(x, jnp.int32(n))


def project_block(before, own, after, mask, row_high, row_low, col_high, col_low):
    lane = lax.broadcasted_iota(jnp.int32, own.shape, 1)
    side = jnp.where(lane < BS // 2, after, before)
    high, low = split(jnp.concatenate([own, side], axis=1))
    dot = functools.partial(jnp.dot, preferred_element_type=jnp.float32)
    along = dot(high, col_high[...]) + (dot(low, col_high[...]) + dot(high, col_low[...]))
    high, low = split(along)
    filtered = dot(row_high[...], high) + (dot(row_high[...], low) + dot(row_low[...], high))
    lower = float(np.tanh(np.float32(SHARPNESS * THRESHOLD)))
    upper = float(np.tanh(np.float32(SHARPNESS * (1.0 - THRESHOLD))))
    return (lower + jnp.tanh(SHARPNESS * (filtered - THRESHOLD))) * (mask.astype(jnp.float32) / (lower + upper))


def upto_lane(x):
    lane = lax.broadcasted_iota(jnp.int32, x.shape, 1)
    step = 1
    while step < x.shape[1]:
        x = x + jnp.where(lane >= step, pltpu.roll(x, step, 1), 0)
        step *= 2
    return x


def locate(wanted, mask_rows, mask_cols, col_count):
    block_row, block_col = over(wanted, mask_cols * col_count)
    row_dev, row_in = over(block_row, mask_rows)
    col_dev, col_in = over(block_col, mask_cols)
    return row_dev * col_count + col_dev, row_in * mask_cols + col_in


def pick(chosen, rank, values, capacity):
    return [
        jnp.sum(jnp.where(chosen & (rank == k + 1), values, 0), axis=1, keepdims=True) for k in range(capacity)
    ]


def matches(rows, capacity):
    before, total = 0, None
    for chosen, values in rows:
        rank = upto_lane(chosen.astype(jnp.int32)) + before
        before = rank[:, BS - 1 :]
        found = [pick(chosen, rank, value, capacity) for value in values]
        total = found if total is None else [[a + b for a, b in zip(x, y)] for x, y in zip(total, found)]
    return total


def active_first(local, masks):
    lane = lax.broadcasted_iota(jnp.int32, masks[0].shape, 1)
    active = []
    for column in local:
        parts = [jnp.where(lane + j * BS == column, mask, 0) for j, mask in enumerate(masks)]
        active.append(sum(jnp.sum(part, axis=1, keepdims=True) for part in parts))
    count = sum(active)
    ahead, behind, places = jnp.zeros_like(count), count, []
    for one in active:
        places.append(jnp.where(one > 0, ahead, behind))
        ahead, behind = ahead + one, behind + 1 - one
    return places, count


def spread(places, columns, lane):
    return sum(jnp.where(lane == at, column, 0) for at, column in zip(places, columns))


def upto_row(x):
    row = lax.broadcasted_iota(jnp.int32, x.shape, 0)
    step = 1
    while step < x.shape[0]:
        x = x + jnp.where(row >= step, pltpu.roll(x, step, 0), 0)
        step *= 2
    return x


def exchange_kernel(
    sizes, mask_rows, mask_cols, spare, density, known,
    arrived, volume, slots, most, padded, outgoing, total, sums, order, table, rh, rl, ch, cl,
    strip_out, strip_in, rows_out, rows_in, tile, tiles, spare_out, spare_in, relay_out, plan_in, plan, load_sem,
    side_send, side_recv, send_sem, recv_sem, sum_send, sum_recv, tile_send, tile_recv, relay_send, relay_recv, hand_sem,
):
    row_count, col_count = sizes
    devices, capacity = outgoing.shape[:2]
    direct = capacity - relay_out.shape[1] if spare else capacity
    group = min(GROUP, capacity)
    bands_of_rows, _, width = density.shape
    height = bands_of_rows * RADIUS
    last = bands_of_rows + 1
    per = (known.shape[0] - 8) // devices
    row, col = lax.axis_index("row"), lax.axis_index("col")
    me = row * col_count + col
    half, quarter = col_count // 2, col_count // 4
    near = quarter * row_count

    def place_of(device):
        return (device // col_count, device % col_count)

    def flip(x, by):
        out, bit = 0, 1
        while bit < max(row_count, col_count):
            out = out + (x // bit + by // bit) % 2 * bit
            bit *= 2
        return out

    def far(i):
        return flip(row, i // half) * col_count + flip(col, half + i % half)

    def beside(i):
        return flip(row, i // quarter) * col_count + flip(col, quarter + i % quarter)

    def close(i):
        return flip(row, i // quarter) * col_count + flip(col, i % quarter)

    def mate(i):
        late = i // near
        return (1 - late) * beside(i % near) + late * close((i + 1) % near)

    partner = far(0)
    side = col // quarter
    outer = (side // 3) + (3 - side) // 3

    def task(t):
        second, late = t // near % 2, t // (2 * near)
        i = t % near
        is_far = (1 - late) * (outer * second + (1 - outer)) + late * outer * (1 - second)
        is_beside = outer * (1 - late) * (1 - second) + (1 - outer) * late * (1 - second)
        far_at = i + near * (outer * late + (1 - outer) * second)
        device = is_far * far(far_at) + is_beside * beside(i) + (1 - is_far - is_beside) * close((i + 1) % near)
        return device, is_far * direct + (1 - is_far) * capacity

    def send(device, k, n=0):
        part = pl.ds(k, n or group)
        return pltpu.make_async_remote_copy(
            src_ref=outgoing.at[device, part], dst_ref=arrived.at[me, part], send_sem=send_sem.at[device],
            recv_sem=recv_sem.at[me], device_id=place_of(device), device_id_type=MESH,
        )

    def receive(device, count):
        part = pl.ds(0, count)
        return pltpu.make_async_remote_copy(
            src_ref=outgoing.at[device, part], dst_ref=arrived.at[device, part], send_sem=send_sem.at[device],
            recv_sem=recv_sem.at[device], device_id=place_of(device), device_id_type=MESH,
        )

    def tile_copy(device, source):
        return pltpu.make_async_remote_copy(
            src_ref=tile, dst_ref=tiles.at[source], send_sem=tile_send.at[device],
            recv_sem=tile_recv.at[source], device_id=place_of(device), device_id_type=MESH,
        )

    def spare_copy(p, count):
        part = pl.ds(p, count)
        return pltpu.make_async_remote_copy(
            src_ref=spare_out.at[part], dst_ref=spare_in.at[part], send_sem=hand_sem.at[0],
            recv_sem=hand_sem.at[1], device_id=place_of(partner), device_id_type=MESH,
        )

    def plan_copy():
        return pltpu.make_async_remote_copy(
            src_ref=order.at[pl.ds(0, devices)], dst_ref=plan_in, send_sem=hand_sem.at[2],
            recv_sem=hand_sem.at[3], device_id=place_of(partner), device_id_type=MESH,
        )

    def relay_copy(i, device, source):
        return pltpu.make_async_remote_copy(
            src_ref=relay_out.at[i], dst_ref=arrived.at[source, pl.ds(direct, capacity - direct)],
            send_sem=relay_send.at[device], recv_sem=relay_recv.at[source], device_id=place_of(device),
            device_id_type=MESH,
        )

    def send_sum(device):
        return pltpu.make_async_remote_copy(
            src_ref=sums.at[me], dst_ref=sums.at[me], send_sem=sum_send.at[device],
            recv_sem=sum_recv.at[me], device_id=place_of(device), device_id_type=MESH,
        )

    def receive_sum(device):
        return pltpu.make_async_remote_copy(
            src_ref=sums.at[me], dst_ref=sums.at[device], send_sem=sum_send.at[device],
            recv_sem=sum_recv.at[device], device_id=place_of(device), device_id_type=MESH,
        )

    def side_copy(dr, dc):
        at = SIDES.index((dr, dc))
        edge, goal_band = {-1: 0, 1: bands_of_rows - 1}, {-1: last, 1: 0}
        cols = {-1: pl.ds(0, BS), 1: pl.ds(width - BS, BS)}
        goal_col = {-1: mask_cols + 1, 1: 0}
        if dr == 0:
            source, goal = strip_out.at[(dc + 1) // 2], strip_in.at[(dc + 1) // 2]
        elif dc == 0:
            source, goal = rows_out.at[(dr + 1) // 2], rows_in.at[(dr + 1) // 2]
        else:
            source, goal = density.at[edge[dr], :, cols[dc]], padded.at[goal_col[dc], goal_band[dr]]
        return pltpu.make_async_remote_copy(
            src_ref=source, dst_ref=goal, send_sem=side_send.at[at], recv_sem=side_recv.at[at],
            device_id=(row + dr, col + dc), device_id_type=MESH,
        )

    def there(dr, dc):
        return (row + dr >= 0) & (row + dr < row_count) & (col + dc >= 0) & (col + dc < col_count)

    barrier = pltpu.get_barrier_semaphore()

    @pl.loop(1, devices)
    def _(o):
        pl.semaphore_signal(barrier, inc=1, device_id=place_of((me + o) % devices), device_id_type=MESH)

    def load(c, sem):
        source = density.at[:, :, pl.ds(pl.multiple_of(c * BS, BS), BS)]
        return pltpu.make_async_copy(source, padded.at[c + 1, pl.ds(1, bands_of_rows)], load_sem.at[sem])

    edges = [load(0, 0), load(mask_cols - 1, 1)]
    rows = [
        pltpu.make_async_copy(density.at[at], rows_out.at[side], load_sem.at[3 + side])
        for side, at in enumerate((0, bands_of_rows - 1))
    ]
    for copy in edges + rows:
        copy.start()

    @pl.loop(1, mask_cols - 1)
    def _(c):
        load(c, 2).start()

    total[...] = jnp.zeros_like(total)

    @pl.when(row == 0)
    def _():
        padded[:, 0] = jnp.zeros((mask_cols + 2, RADIUS, BS), jnp.float32)

    @pl.when(row == row_count - 1)
    def _():
        padded[:, last] = jnp.zeros((mask_cols + 2, RADIUS, BS), jnp.float32)

    @pl.when(col == 0)
    def _():
        padded[0] = jnp.zeros(padded.shape[1:], jnp.float32)

    @pl.when(col == col_count - 1)
    def _():
        padded[mask_cols + 1] = jnp.zeros(padded.shape[1:], jnp.float32)

    piece = height // STRIP
    parts = piece // RADIUS
    spot, _ = over(lax.broadcasted_iota(jnp.int32, (piece, BS), 1), RADIUS)
    for side, copy in enumerate(edges):
        copy.wait()
        strip = jnp.zeros((piece, BS), jnp.float32)
        for p in range(STRIP):
            edge = padded[1 + side * (mask_cols - 1), pl.ds(1 + p * parts, parts)].reshape(piece, BS)
            strip = jnp.where(spot == p, pltpu.roll(edge, (p * RADIUS + side * RADIUS) % BS, 1), strip)
        strip_out[side] = strip

    for copy in rows:
        copy.wait()
    pl.semaphore_wait(barrier, devices - 1)
    for dr, dc in SIDES:

        @pl.when(there(dr, dc))
        def _():
            side_copy(dr, dc).start()

    shape = (devices, BS)
    device_of, lane = (lax.broadcasted_iota(jnp.int32, shape, d) for d in range(2))
    rows_of = []
    for j in range(per):
        source, local = locate(known[pl.ds(j, devices, stride=per)], mask_rows, mask_cols, col_count)
        rows_of.append((source == me, [local]))
    (local,) = matches(rows_of, capacity)
    masks = [jnp.broadcast_to(known[devices * per + j : devices * per + j + 1], shape) for j in range(per)]
    places, count = active_first(local, masks)
    sorted_local = spread(places, local, lane)
    in_rank = (lane >= capacity) & (lane < 2 * capacity) & (lane - capacity < count)
    order[0:devices] = sorted_local + jnp.where(in_rank, 1, 0)
    order[devices:] = jnp.zeros((8, BS), jnp.int32)
    tile[...] = known[devices * per : devices * per + per]
    if spare:
        _, at_col = over(device_of, col_count)
        away = over(at_col, half)[0] != col // half
        extra = [(away & (count > k)).astype(jnp.int32) for k in range(direct, capacity)]
        upto = upto_row(sum(extra))
        at = upto - sum(extra)
        lists, hand = jnp.zeros((1, BS), jnp.int32), jnp.zeros(shape, jnp.int32)
        for k, one in zip(range(direct, capacity), extra):
            picked = jnp.sum(jnp.where(lane == k, sorted_local, 0), axis=1, keepdims=True)
            lists = lists + jnp.sum(jnp.where((one > 0) & (at == lane), picked, 0), axis=0, keepdims=True)
            held = jnp.where((one > 0) & (at < spare), at, spare)
            hand = hand + jnp.where(lane == 2 * capacity + k, held, 0)
            at = at + one
        full = upto[devices - 1 :]
        order[0:devices] = order[0:devices] + hand
        order[devices : devices + 1] = lists
        order[devices + 1 : devices + 2] = (lane[0:1] < full).astype(jnp.int32)
        tile[...] = tile[...] + 2 * full
        spare_in[spare] = jnp.zeros((BS, BS), jnp.bfloat16)
    to_scalars = pltpu.make_async_copy(order, table, load_sem.at[5])
    to_scalars.start()
    rh[...], rl[...] = row_bands()
    ch[...], cl[...] = col_bands()
    for dr, dc in SIDES:

        @pl.when(there(-dr, -dc))
        def _():
            side_copy(dr, dc).wait_recv()
            if dr == 0:
                strip = strip_in[(dc + 1) // 2]
                for p in range(STRIP):
                    shift = (BS - p * RADIUS - (dc + 1) // 2 * RADIUS) % BS
                    moved = pltpu.roll(strip, shift, 1).reshape(parts, RADIUS, BS)
                    padded[0 if dc == 1 else mask_cols + 1, pl.ds(1 + p * parts, parts)] = moved
            elif dc == 0:
                for c in range(mask_cols):
                    padded[c + 1, 0 if dr == 1 else last] = rows_in[(dr + 1) // 2, :, pl.ds(c * BS, BS)]

        @pl.when(there(dr, dc))
        def _():
            side_copy(dr, dc).wait_send()

    middle = padded.at[pl.ds(2, mask_cols - 2), pl.ds(1, bands_of_rows)]
    pltpu.make_async_copy(middle, middle, load_sem.at[2]).wait()
    to_scalars.wait()


    @pl.loop(1, devices)
    def _(o):
        tile_copy((me + o) % devices, me).start()

    tiles[me] = tile[...]
    if spare:
        plan_copy().start()

    def block(local, active):
        r, c = over(local, mask_cols)
        deep = BS // RADIUS
        before, own, after = (
            jnp.concatenate([padded[c + i, r * deep + j] for j in range(deep + 2)], axis=0) for i in range(3)
        )
        return project_block(before, own, after, active, rh, rl, ch, cl)

    def turn(device, blocks, pending, opening):
        @pl.loop(0, lax.div(blocks, group))
        def _(p):
            cells = []
            for k in range(group):
                active = table[device, capacity + p * group + k]
                cells.append(block(table[device, p * group + k], active))
                outgoing[device, p * group + k] = cells[k].astype(jnp.bfloat16)
            total[...] += sum(cells)
            pl.when(p == 0)(pending)

            @pl.when((p > 0) & opening)
            def _():
                send(device, (p - 1) * group).start()

    def follow(before):
        device, blocks = before
        if direct == capacity:
            send(device, 0, capacity).start()
            return
        pl.when(blocks == direct)(lambda: send(device, 0, direct).start())
        pl.when(blocks == capacity)(lambda: send(device, 0, capacity).start())

    def steps(start, stop, first, before):
        def step(t, before):
            device, blocks = task(t)

            def pending():
                pl.when(t == start)(first)
                if start == 0:
                    pl.when(t == 1)(lambda: send(before[0], before[1] - group).start())
                pl.when(t > max(start, 1))(lambda: follow(before))

            turn(device, blocks, pending, t == 0)
            return device, blocks

        return lax.fori_loop(start, stop, step, before)

    def relay():
        plan_copy().wait()
        to_plan = pltpu.make_async_copy(plan_in, plan, load_sem.at[0])
        to_plan.start()
        to_plan.wait()
        spare_copy(0, spare).wait()

        @pl.loop(0, 2 * near)
        def _(i):
            for k in range(direct, capacity):
                relay_out[i, k - direct] = spare_in[plan[mate(i), 2 * capacity + k]]

            @pl.when(i > 0)
            def _():
                relay_copy(i - 1, mate(i - 1), partner).start()

        arrived[partner, direct:] = relay_out[2 * near - 1]

    before = steps(0, near, lambda: None, (me, capacity))
    if spare:

        @pl.loop(0, spare // group)
        def _(p):
            cells = []
            for k in range(group):
                cells.append(block(table[devices, p * group + k], table[devices + 1, p * group + k]))
                spare_out[p * group + k] = cells[k].astype(jnp.bfloat16)
            total[...] += sum(cells)
            pl.when(p == 0)(lambda: follow(before))

            @pl.when(p > 0)
            def _():
                spare_copy((p - 1) * group, group).start()

        before = steps(near, 2 * near, lambda: spare_copy(spare - group, group).start(), before)
        pl.when(outer == 1)(relay)
        steps(2 * near, 4 * near, lambda: follow(before), before)
        pl.when(outer == 0)(relay)
    else:
        steps(near, 4 * near, lambda: follow(before), before)

    sums[me] = jnp.sum(total[...], axis=0, keepdims=True)
    arrived[me] = outgoing[me]

    @pl.loop(1, devices)
    def _(o):
        send_sum((me + o) % devices).start()

    @pl.loop(1, devices)
    def _(o):
        other = (me + o) % devices
        tile_copy(other, other).wait()

    rows_in_order = []
    for j in range(per):
        mine = jnp.broadcast_to(known[pl.ds(me * per + j, 1)], shape)
        source, local = locate(mine, mask_rows, mask_cols, col_count)
        rows_in_order.append((source == device_of, [local, lane + j * BS]))
    local, slot = matches(rows_in_order, capacity)
    places, _ = active_first(local, [tiles[:, j] & 1 for j in range(per)])
    slots[...] = spread(places, slot, lane)
    most[...] = jnp.max(tiles[:, 0] >> 1, axis=0, keepdims=True)

    @pl.loop(0, 2 * near)
    def _(i):
        receive(far(i), direct).wait()

    @pl.loop(0, 2 * near - 1)
    def _(i):
        receive(mate(i), capacity).wait()

    if spare:

        @pl.loop(0, 2 * near - 1)
        def _(i):
            relay_copy(i, mate(i), partner).wait_send()
            relay_copy(i, mate(i), far(i + 1)).wait_recv()

    @pl.loop(1, devices)
    def _(o):
        other = (me + o) % devices
        send_sum(other).wait_send()
        receive_sum(other).wait_recv()

    volume[...] = jnp.sum(sums[...], axis=0)


def exchange(mask_shape, density, known, sizes, lean):
    devices = sizes[0] * sizes[1]
    capacity = mask_shape[0] * mask_shape[1] // devices
    extra = capacity // 4
    lean = lean and extra > 0
    spare = (devices // 2 + SLACK) // GROUP * GROUP if lean else 0
    height, width = density.shape
    in_hbm = pl.BlockSpec(memory_space=pltpu.HBM)
    whole = pl.BlockSpec(memory_space=pltpu.VMEM)
    cells = devices * capacity * BS * BS
    strips = pltpu.VMEM((2, height // STRIP, BS), jnp.float32)
    rows = pltpu.VMEM((2, RADIUS, width), jnp.float32)
    row_band = pltpu.VMEM((BS, BS + 2 * RADIUS), jnp.bfloat16)
    col_band = pltpu.VMEM((2 * BS, BS), jnp.bfloat16)
    plan = (devices, BS)
    per = devices * capacity // BS
    blocks = lambda *n: pltpu.VMEM((*n, BS, BS), jnp.bfloat16)
    return pl.pallas_call(
        functools.partial(exchange_kernel, sizes, *mask_shape, spare),
        out_shape=(
            jax.ShapeDtypeStruct((devices, capacity, BS, BS), jnp.bfloat16),
            jax.ShapeDtypeStruct((1, BS), jnp.float32),
            jax.ShapeDtypeStruct(plan, jnp.int32),
            jax.ShapeDtypeStruct((1, BS), jnp.int32),
        ),
        in_specs=[in_hbm, whole],
        out_specs=(whole, whole, whole, whole),
        scratch_shapes=[
            pltpu.VMEM((width // BS + 2, height // RADIUS + 2, RADIUS, BS), jnp.float32),
            blocks(devices, capacity),
            pltpu.VMEM((BS, BS), jnp.float32),
            pltpu.VMEM((devices, 1, BS), jnp.float32),
            pltpu.VMEM((devices + 8, BS), jnp.int32),
            pltpu.SMEM((devices + 8, BS), jnp.int32),
            row_band,
            row_band,
            col_band,
            col_band,
            strips,
            strips,
            rows,
            rows,
            pltpu.VMEM((per, BS), jnp.int32),
            pltpu.VMEM((devices, per, BS), jnp.int32),
            blocks(max(spare, 1)),
            blocks(spare + 1),
            blocks(devices // 2 if lean else 1, max(extra, 1)),
            pltpu.VMEM(plan, jnp.int32),
            pltpu.SMEM(plan, jnp.int32),
            pltpu.SemaphoreType.DMA((6,)),
            pltpu.SemaphoreType.DMA((len(SIDES),)),
            pltpu.SemaphoreType.DMA((len(SIDES),)),
        ]
        + [pltpu.SemaphoreType.DMA((devices,))] * 8
        + [pltpu.SemaphoreType.DMA((4,))],
        compiler_params=pltpu.CompilerParams(
            vmem_limit_bytes=44 * MIB, collective_id=0 if lean else 1, has_side_effects=True
        ),
        cost_estimate=pl.CostEstimate(flops=cells * 2000, bytes_accessed=density.size * 4, transcendentals=cells),
        name="exchange_lean" if lean else "exchange",
    )(density.reshape(height // RADIUS, RADIUS, width), known), spare


def place_kernel(cells, slots, arrived, volume, out, constraint, store_sem):
    devices, capacity = arrived.shape[:2]

    @pl.loop(0, devices)
    def _(d):
        for k in range(capacity):
            pltpu.make_async_copy(arrived.at[d, k], out.at[slots[d, k]], store_sem).start()

    mean = jnp.sum(volume[...], keepdims=True) / cells
    constraint[...] = mean / VOLUME_TARGET - 1.0
    landed = out.at[pl.ds(0, devices * capacity)]
    pltpu.make_async_copy(landed, landed, store_sem).wait()


def place(slots, arrived, volume, cells):
    count = arrived.shape[0] * arrived.shape[1]
    whole = pl.BlockSpec(memory_space=pltpu.VMEM)
    return pl.pallas_call(
        functools.partial(place_kernel, cells),
        out_shape=(
            jax.ShapeDtypeStruct((count, BS, BS), jnp.bfloat16),
            jax.ShapeDtypeStruct((1, 1), jnp.float32),
        ),
        in_specs=[pl.BlockSpec(memory_space=pltpu.SMEM), whole, whole],
        out_specs=(pl.BlockSpec(memory_space=pltpu.HBM), whole),
        scratch_shapes=[pltpu.SemaphoreType.DMA],
        compiler_params=pltpu.CompilerParams(vmem_limit_bytes=8 * MIB),
        cost_estimate=pl.CostEstimate(flops=0, bytes_accessed=2 * arrived.size * 2, transcendentals=0),
        name="place",
    )(slots, arrived, volume)


def per_device(density, design_mask, rebalance):
    sizes = (lax.axis_size("row"), lax.axis_size("col"))
    shape = design_mask.shape
    cells = float(density.size * sizes[0] * sizes[1])
    flat = design_mask.reshape(-1, BS)
    known = jnp.concatenate([rebalance.reshape(-1, BS), jnp.pad(flat, ((0, 8 - flat.shape[0]), (0, 0)))])

    def full():
        (arrived, volume, slots, _), _ = exchange(shape, density, known, sizes, False)
        return place(slots, arrived, volume, cells)

    if design_mask.size // (sizes[0] * sizes[1]) < 4:
        balanced, constraint = full()
        return balanced, constraint[0, 0]
    (arrived, volume, slots, most), spare = exchange(shape, density, known, sizes, True)
    balanced, constraint = lax.cond(most[0, 0] > spare, full, lambda: place(slots, arrived, volume, cells))
    return balanced, constraint[0, 0]


def solution(mesh):
    return jax.shard_map(
        per_device,
        mesh=mesh,
        in_specs=(P("row", "col"), P("row", "col"), P()),
        out_specs=(P(("row", "col"), None, None), P()),
        check_vma=False,
    )
```

```python
import functools

import jax
import jax.numpy as jnp
import numpy as np
from jax import lax
from jax.experimental import pallas as pl
from jax.experimental.pallas import tpu as pltpu
from jax.sharding import PartitionSpec as P

BS = 128
RADIUS = 16
SHARPNESS = 32.0
THRESHOLD = 0.5
VOLUME_TARGET = 0.4
MESH = pl.DeviceIdType.MESH
MIB = 2**20
GROUP = 2
SLACK = 2
STRIP = BS // RADIUS
SIDES = [(dr, dc) for dr in (-1, 0, 1) for dc in (-1, 0, 1) if dr or dc]


def filter_taps():
    sigma = RADIUS / 4.0
    offsets = np.arange(2 * RADIUS + 1, dtype=np.float64) - RADIUS
    raw_taps = np.exp(-offsets * offsets / (2.0 * sigma * sigma))
    return (raw_taps / raw_taps.sum()).astype(np.float32)


def split(x):
    high = x.astype(jnp.bfloat16)
    return high, (x - high.astype(jnp.float32)).astype(jnp.bfloat16)


def band(distance):
    taps = filter_taps()
    weight = jnp.zeros(distance.shape, jnp.float32)
    for far in range(RADIUS + 1):
        weight = jnp.where(distance == far, float(taps[RADIUS + far]), weight)
    return split(weight)


def col_bands():
    source = lax.broadcasted_iota(jnp.int32, (2 * BS, BS), 0)
    source = jnp.where(source < BS + BS // 2, source, source - 2 * BS)
    return band(jnp.abs(source - lax.broadcasted_iota(jnp.int32, source.shape, 1)))


def row_bands():
    source = lax.broadcasted_iota(jnp.int32, (BS, BS + 2 * RADIUS), 1) - RADIUS
    return band(jnp.abs(source - lax.broadcasted_iota(jnp.int32, source.shape, 0)))


def over(x, n):
    if n & (n - 1) == 0:
        return x >> (n.bit_length() - 1), x & (n - 1)
    return lax.div(x, jnp.int32(n)), lax.rem(x, jnp.int32(n))


def project_block(before, own, after, mask, row_high, row_low, col_high, col_low):
    lane = lax.broadcasted_iota(jnp.int32, own.shape, 1)
    side = jnp.where(lane < BS // 2, after, before)
    high, low = split(jnp.concatenate([own, side], axis=1))
    dot = functools.partial(jnp.dot, preferred_element_type=jnp.float32)
    along = dot(high, col_high[...]) + (dot(low, col_high[...]) + dot(high, col_low[...]))
    high, low = split(along)
    filtered = dot(row_high[...], high) + (dot(row_high[...], low) + dot(row_low[...], high))
    lower = float(np.tanh(np.float32(SHARPNESS * THRESHOLD)))
    upper = float(np.tanh(np.float32(SHARPNESS * (1.0 - THRESHOLD))))
    return (lower + jnp.tanh(SHARPNESS * (filtered - THRESHOLD))) * (mask.astype(jnp.float32) / (lower + upper))


def upto_lane(x):
    lane = lax.broadcasted_iota(jnp.int32, x.shape, 1)
    step = 1
    while step < x.shape[1]:
        x = x + jnp.where(lane >= step, pltpu.roll(x, step, 1), 0)
        step *= 2
    return x


def locate(wanted, mask_rows, mask_cols, col_count):
    block_row, block_col = over(wanted, mask_cols * col_count)
    row_dev, row_in = over(block_row, mask_rows)
    col_dev, col_in = over(block_col, mask_cols)
    return row_dev * col_count + col_dev, row_in * mask_cols + col_in


def pick(chosen, rank, values, capacity):
    return [
        jnp.sum(jnp.where(chosen & (rank == k + 1), values, 0), axis=1, keepdims=True) for k in range(capacity)
    ]


def matches(rows, capacity):
    before, total = 0, None
    for chosen, values in rows:
        rank = upto_lane(chosen.astype(jnp.int32)) + before
        before = rank[:, BS - 1 :]
        found = [pick(chosen, rank, value, capacity) for value in values]
        total = found if total is None else [[a + b for a, b in zip(x, y)] for x, y in zip(total, found)]
    return total


def active_first(local, masks):
    lane = lax.broadcasted_iota(jnp.int32, masks[0].shape, 1)
    active = []
    for column in local:
        parts = [jnp.where(lane + j * BS == column, mask, 0) for j, mask in enumerate(masks)]
        active.append(sum(jnp.sum(part, axis=1, keepdims=True) for part in parts))
    count = sum(active)
    ahead, behind, places = jnp.zeros_like(count), count, []
    for one in active:
        places.append(jnp.where(one > 0, ahead, behind))
        ahead, behind = ahead + one, behind + 1 - one
    return places, count


def spread(places, columns, lane):
    return sum(jnp.where(lane == at, column, 0) for at, column in zip(places, columns))


def upto_row(x):
    row = lax.broadcasted_iota(jnp.int32, x.shape, 0)
    step = 1
    while step < x.shape[0]:
        x = x + jnp.where(row >= step, pltpu.roll(x, step, 0), 0)
        step *= 2
    return x


def exchange_kernel(
    sizes, mask_rows, mask_cols, spare, density, known,
    arrived, volume, slots, most, padded, outgoing, total, sums, order, table, rh, rl, ch, cl,
    strip_out, strip_in, rows_out, rows_in, tile, tiles, spare_out, spare_in, relay_out, plan_in, plan, load_sem,
    side_send, side_recv, send_sem, recv_sem, sum_send, sum_recv, tile_send, tile_recv, relay_send, relay_recv, hand_sem,
):
    row_count, col_count = sizes
    devices, capacity = outgoing.shape[:2]
    direct = capacity - relay_out.shape[1] if spare else capacity
    group = min(GROUP, capacity)
    bands_of_rows, _, width = density.shape
    height = bands_of_rows * RADIUS
    last = bands_of_rows + 1
    per = (known.shape[0] - 8) // devices
    row, col = lax.axis_index("row"), lax.axis_index("col")
    me = row * col_count + col
    half, quarter = col_count // 2, col_count // 4
    near = quarter * row_count

    def place_of(device):
        return (device // col_count, device % col_count)

    def flip(x, by):
        out, bit = 0, 1
        while bit < max(row_count, col_count):
            out = out + (x // bit + by // bit) % 2 * bit
            bit *= 2
        return out

    def far(i):
        return flip(row, i // half) * col_count + flip(col, half + i % half)

    def beside(i):
        return flip(row, i // quarter) * col_count + flip(col, quarter + i % quarter)

    def close(i):
        return flip(row, i // quarter) * col_count + flip(col, i % quarter)

    def mate(i):
        late = i // near
        return (1 - late) * beside(i % near) + late * close((i + 1) % near)

    partner = far(0)
    side = col // quarter
    outer = (side // 3) + (3 - side) // 3

    def task(t):
        second, late = t // near % 2, t // (2 * near)
        i = t % near
        same = outer * second + (1 - outer) * (1 - second)
        is_far = (1 - late) * same + late * (1 - second)
        is_beside = (1 - late) * (1 - same)
        far_at = i + near * late
        device = is_far * far(far_at) + is_beside * beside(i) + (1 - is_far - is_beside) * close((i + 1) % near)
        return device, is_far * direct + (1 - is_far) * capacity

    def send(device, k, n=0):
        part = pl.ds(k, n or group)
        return pltpu.make_async_remote_copy(
            src_ref=outgoing.at[device, part], dst_ref=arrived.at[me, part], send_sem=send_sem.at[device],
            recv_sem=recv_sem.at[me], device_id=place_of(device), device_id_type=MESH,
        )

    def receive(device, count):
        part = pl.ds(0, count)
        return pltpu.make_async_remote_copy(
            src_ref=outgoing.at[device, part], dst_ref=arrived.at[device, part], send_sem=send_sem.at[device],
            recv_sem=recv_sem.at[device], device_id=place_of(device), device_id_type=MESH,
        )

    def tile_copy(device, source):
        return pltpu.make_async_remote_copy(
            src_ref=tile, dst_ref=tiles.at[source], send_sem=tile_send.at[device],
            recv_sem=tile_recv.at[source], device_id=place_of(device), device_id_type=MESH,
        )

    def spare_copy(p, count):
        part = pl.ds(p, count)
        return pltpu.make_async_remote_copy(
            src_ref=spare_out.at[part], dst_ref=spare_in.at[part], send_sem=hand_sem.at[0],
            recv_sem=hand_sem.at[1], device_id=place_of(partner), device_id_type=MESH,
        )

    def plan_copy():
        return pltpu.make_async_remote_copy(
            src_ref=order.at[pl.ds(0, devices)], dst_ref=plan_in, send_sem=hand_sem.at[2],
            recv_sem=hand_sem.at[3], device_id=place_of(partner), device_id_type=MESH,
        )

    def relay_copy(i, device, source):
        return pltpu.make_async_remote_copy(
            src_ref=relay_out.at[i], dst_ref=arrived.at[source, pl.ds(direct, capacity - direct)],
            send_sem=relay_send.at[device], recv_sem=relay_recv.at[source], device_id=place_of(device),
            device_id_type=MESH,
        )

    def send_sum(device):
        return pltpu.make_async_remote_copy(
            src_ref=sums.at[me], dst_ref=sums.at[me], send_sem=sum_send.at[device],
            recv_sem=sum_recv.at[me], device_id=place_of(device), device_id_type=MESH,
        )

    def receive_sum(device):
        return pltpu.make_async_remote_copy(
            src_ref=sums.at[me], dst_ref=sums.at[device], send_sem=sum_send.at[device],
            recv_sem=sum_recv.at[device], device_id=place_of(device), device_id_type=MESH,
        )

    def side_copy(dr, dc):
        at = SIDES.index((dr, dc))
        edge, goal_band = {-1: 0, 1: bands_of_rows - 1}, {-1: last, 1: 0}
        cols = {-1: pl.ds(0, BS), 1: pl.ds(width - BS, BS)}
        goal_col = {-1: mask_cols + 1, 1: 0}
        if dr == 0:
            source, goal = strip_out.at[(dc + 1) // 2], strip_in.at[(dc + 1) // 2]
        elif dc == 0:
            source, goal = rows_out.at[(dr + 1) // 2], rows_in.at[(dr + 1) // 2]
        else:
            source, goal = density.at[edge[dr], :, cols[dc]], padded.at[goal_col[dc], goal_band[dr]]
        return pltpu.make_async_remote_copy(
            src_ref=source, dst_ref=goal, send_sem=side_send.at[at], recv_sem=side_recv.at[at],
            device_id=(row + dr, col + dc), device_id_type=MESH,
        )

    def there(dr, dc):
        return (row + dr >= 0) & (row + dr < row_count) & (col + dc >= 0) & (col + dc < col_count)

    barrier = pltpu.get_barrier_semaphore()

    @pl.loop(1, devices)
    def _(o):
        pl.semaphore_signal(barrier, inc=1, device_id=place_of((me + o) % devices), device_id_type=MESH)

    def load(c, sem):
        source = density.at[:, :, pl.ds(pl.multiple_of(c * BS, BS), BS)]
        return pltpu.make_async_copy(source, padded.at[c + 1, pl.ds(1, bands_of_rows)], load_sem.at[sem])

    edges = [load(0, 0), load(mask_cols - 1, 1)]
    rows = [
        pltpu.make_async_copy(density.at[at], rows_out.at[side], load_sem.at[3 + side])
        for side, at in enumerate((0, bands_of_rows - 1))
    ]
    for copy in edges + rows:
        copy.start()

    @pl.loop(1, mask_cols - 1)
    def _(c):
        load(c, 2).start()

    total[...] = jnp.zeros_like(total)

    @pl.when(row == 0)
    def _():
        padded[:, 0] = jnp.zeros((mask_cols + 2, RADIUS, BS), jnp.float32)

    @pl.when(row == row_count - 1)
    def _():
        padded[:, last] = jnp.zeros((mask_cols + 2, RADIUS, BS), jnp.float32)

    @pl.when(col == 0)
    def _():
        padded[0] = jnp.zeros(padded.shape[1:], jnp.float32)

    @pl.when(col == col_count - 1)
    def _():
        padded[mask_cols + 1] = jnp.zeros(padded.shape[1:], jnp.float32)

    piece = height // STRIP
    parts = piece // RADIUS
    spot, _ = over(lax.broadcasted_iota(jnp.int32, (piece, BS), 1), RADIUS)
    for side, copy in enumerate(edges):
        copy.wait()
        strip = jnp.zeros((piece, BS), jnp.float32)
        for p in range(STRIP):
            edge = padded[1 + side * (mask_cols - 1), pl.ds(1 + p * parts, parts)].reshape(piece, BS)
            strip = jnp.where(spot == p, pltpu.roll(edge, (p * RADIUS + side * RADIUS) % BS, 1), strip)
        strip_out[side] = strip

    for copy in rows:
        copy.wait()
    pl.semaphore_wait(barrier, devices - 1)
    for dr, dc in SIDES:

        @pl.when(there(dr, dc))
        def _():
            side_copy(dr, dc).start()

    shape = (devices, BS)
    device_of, lane = (lax.broadcasted_iota(jnp.int32, shape, d) for d in range(2))
    rows_of = []
    for j in range(per):
        source, local = locate(known[pl.ds(j, devices, stride=per)], mask_rows, mask_cols, col_count)
        rows_of.append((source == me, [local]))
    (local,) = matches(rows_of, capacity)
    masks = [jnp.broadcast_to(known[devices * per + j : devices * per + j + 1], shape) for j in range(per)]
    places, count = active_first(local, masks)
    sorted_local = spread(places, local, lane)
    in_rank = (lane >= capacity) & (lane < 2 * capacity) & (lane - capacity < count)
    order[0:devices] = sorted_local + jnp.where(in_rank, 1, 0)
    order[devices:] = jnp.zeros((8, BS), jnp.int32)
    tile[...] = known[devices * per : devices * per + per]
    if spare:
        _, at_col = over(device_of, col_count)
        away = over(at_col, half)[0] != col // half
        extra = [(away & (count > k)).astype(jnp.int32) for k in range(direct, capacity)]
        upto = upto_row(sum(extra))
        at = upto - sum(extra)
        lists, hand = jnp.zeros((1, BS), jnp.int32), jnp.zeros(shape, jnp.int32)
        for k, one in zip(range(direct, capacity), extra):
            picked = jnp.sum(jnp.where(lane == k, sorted_local, 0), axis=1, keepdims=True)
            lists = lists + jnp.sum(jnp.where((one > 0) & (at == lane), picked, 0), axis=0, keepdims=True)
            held = jnp.where((one > 0) & (at < spare), at, spare)
            hand = hand + jnp.where(lane == 2 * capacity + k, held, 0)
            at = at + one
        full = upto[devices - 1 :]
        order[0:devices] = order[0:devices] + hand
        order[devices : devices + 1] = lists
        order[devices + 1 : devices + 2] = (lane[0:1] < full).astype(jnp.int32)
        tile[...] = tile[...] + 2 * full
        spare_in[spare] = jnp.zeros((BS, BS), jnp.bfloat16)
    to_scalars = pltpu.make_async_copy(order, table, load_sem.at[5])
    to_scalars.start()
    rh[...], rl[...] = row_bands()
    ch[...], cl[...] = col_bands()
    for dr, dc in SIDES:

        @pl.when(there(-dr, -dc))
        def _():
            side_copy(dr, dc).wait_recv()
            if dr == 0:
                strip = strip_in[(dc + 1) // 2]
                for p in range(STRIP):
                    shift = (BS - p * RADIUS - (dc + 1) // 2 * RADIUS) % BS
                    moved = pltpu.roll(strip, shift, 1).reshape(parts, RADIUS, BS)
                    padded[0 if dc == 1 else mask_cols + 1, pl.ds(1 + p * parts, parts)] = moved
            elif dc == 0:
                for c in range(mask_cols):
                    padded[c + 1, 0 if dr == 1 else last] = rows_in[(dr + 1) // 2, :, pl.ds(c * BS, BS)]

        @pl.when(there(dr, dc))
        def _():
            side_copy(dr, dc).wait_send()

    middle = padded.at[pl.ds(2, mask_cols - 2), pl.ds(1, bands_of_rows)]
    pltpu.make_async_copy(middle, middle, load_sem.at[2]).wait()
    to_scalars.wait()


    @pl.loop(1, devices)
    def _(o):
        tile_copy((me + o) % devices, me).start()

    tiles[me] = tile[...]
    if spare:
        plan_copy().start()

    def block(local, active):
        r, c = over(local, mask_cols)
        deep = BS // RADIUS
        before, own, after = (
            jnp.concatenate([padded[c + i, r * deep + j] for j in range(deep + 2)], axis=0) for i in range(3)
        )
        return project_block(before, own, after, active, rh, rl, ch, cl)

    def turn(device, blocks, pending, opening):
        @pl.loop(0, lax.div(blocks, group))
        def _(p):
            cells = []
            for k in range(group):
                active = table[device, capacity + p * group + k]
                cells.append(block(table[device, p * group + k], active))
                outgoing[device, p * group + k] = cells[k].astype(jnp.bfloat16)
            total[...] += sum(cells)
            pl.when(p == 0)(pending)

            @pl.when((p > 0) & opening)
            def _():
                send(device, (p - 1) * group).start()

    def follow(before):
        device, blocks = before
        if direct == capacity:
            send(device, 0, capacity).start()
            return
        pl.when(blocks == direct)(lambda: send(device, 0, direct).start())
        pl.when(blocks == capacity)(lambda: send(device, 0, capacity).start())

    def steps(start, stop, first, before):
        def step(t, before):
            device, blocks = task(t)

            def pending():
                pl.when(t == start)(first)
                if start == 0:
                    pl.when(t == 1)(lambda: send(before[0], before[1] - group).start())
                pl.when(t > max(start, 1))(lambda: follow(before))

            turn(device, blocks, pending, t == 0)
            return device, blocks

        return lax.fori_loop(start, stop, step, before)

    def relay():
        plan_copy().wait()
        to_plan = pltpu.make_async_copy(plan_in, plan, load_sem.at[0])
        to_plan.start()
        to_plan.wait()
        spare_copy(0, spare).wait()

        @pl.loop(0, 2 * near)
        def _(i):
            for k in range(direct, capacity):
                relay_out[i, k - direct] = spare_in[plan[mate(i), 2 * capacity + k]]

            @pl.when(i > 0)
            def _():
                relay_copy(i - 1, mate(i - 1), partner).start()

        arrived[partner, direct:] = relay_out[2 * near - 1]

    before = steps(0, near, lambda: None, (me, capacity))
    if spare:

        @pl.loop(0, spare // group)
        def _(p):
            cells = []
            for k in range(group):
                cells.append(block(table[devices, p * group + k], table[devices + 1, p * group + k]))
                spare_out[p * group + k] = cells[k].astype(jnp.bfloat16)
            total[...] += sum(cells)
            pl.when(p == 0)(lambda: follow(before))

            @pl.when(p > 0)
            def _():
                spare_copy((p - 1) * group, group).start()

        before = steps(near, 2 * near, lambda: spare_copy(spare - group, group).start(), before)
        pl.when(outer == 1)(relay)
        steps(2 * near, 4 * near, lambda: follow(before), before)
        pl.when(outer == 0)(relay)
    else:
        steps(near, 4 * near, lambda: follow(before), before)

    sums[me] = jnp.sum(total[...], axis=0, keepdims=True)
    arrived[me] = outgoing[me]

    @pl.loop(1, devices)
    def _(o):
        send_sum((me + o) % devices).start()

    @pl.loop(1, devices)
    def _(o):
        other = (me + o) % devices
        tile_copy(other, other).wait()

    rows_in_order = []
    for j in range(per):
        mine = jnp.broadcast_to(known[pl.ds(me * per + j, 1)], shape)
        source, local = locate(mine, mask_rows, mask_cols, col_count)
        rows_in_order.append((source == device_of, [local, lane + j * BS]))
    local, slot = matches(rows_in_order, capacity)
    places, _ = active_first(local, [tiles[:, j] & 1 for j in range(per)])
    slots[...] = spread(places, slot, lane)
    most[...] = jnp.max(tiles[:, 0] >> 1, axis=0, keepdims=True)

    @pl.loop(0, 2 * near)
    def _(i):
        receive(far(i), direct).wait()

    @pl.loop(0, 2 * near - 1)
    def _(i):
        receive(mate(i), capacity).wait()

    if spare:

        @pl.loop(0, 2 * near - 1)
        def _(i):
            relay_copy(i, mate(i), partner).wait_send()
            relay_copy(i, mate(i), far(i + 1)).wait_recv()

    @pl.loop(1, devices)
    def _(o):
        other = (me + o) % devices
        send_sum(other).wait_send()
        receive_sum(other).wait_recv()

    volume[...] = jnp.sum(sums[...], axis=0)


def exchange(mask_shape, density, known, sizes, lean):
    devices = sizes[0] * sizes[1]
    capacity = mask_shape[0] * mask_shape[1] // devices
    extra = capacity // 4
    lean = lean and extra > 0
    spare = (devices // 2 + SLACK) // GROUP * GROUP if lean else 0
    height, width = density.shape
    in_hbm = pl.BlockSpec(memory_space=pltpu.HBM)
    whole = pl.BlockSpec(memory_space=pltpu.VMEM)
    cells = devices * capacity * BS * BS
    strips = pltpu.VMEM((2, height // STRIP, BS), jnp.float32)
    rows = pltpu.VMEM((2, RADIUS, width), jnp.float32)
    row_band = pltpu.VMEM((BS, BS + 2 * RADIUS), jnp.bfloat16)
    col_band = pltpu.VMEM((2 * BS, BS), jnp.bfloat16)
    plan = (devices, BS)
    per = devices * capacity // BS
    blocks = lambda *n: pltpu.VMEM((*n, BS, BS), jnp.bfloat16)
    return pl.pallas_call(
        functools.partial(exchange_kernel, sizes, *mask_shape, spare),
        out_shape=(
            jax.ShapeDtypeStruct((devices, capacity, BS, BS), jnp.bfloat16),
            jax.ShapeDtypeStruct((1, BS), jnp.float32),
            jax.ShapeDtypeStruct(plan, jnp.int32),
            jax.ShapeDtypeStruct((1, BS), jnp.int32),
        ),
        in_specs=[in_hbm, whole],
        out_specs=(whole, whole, whole, whole),
        scratch_shapes=[
            pltpu.VMEM((width // BS + 2, height // RADIUS + 2, RADIUS, BS), jnp.float32),
            blocks(devices, capacity),
            pltpu.VMEM((BS, BS), jnp.float32),
            pltpu.VMEM((devices, 1, BS), jnp.float32),
            pltpu.VMEM((devices + 8, BS), jnp.int32),
            pltpu.SMEM((devices + 8, BS), jnp.int32),
            row_band,
            row_band,
            col_band,
            col_band,
            strips,
            strips,
            rows,
            rows,
            pltpu.VMEM((per, BS), jnp.int32),
            pltpu.VMEM((devices, per, BS), jnp.int32),
            blocks(max(spare, 1)),
            blocks(spare + 1),
            blocks(devices // 2 if lean else 1, max(extra, 1)),
            pltpu.VMEM(plan, jnp.int32),
            pltpu.SMEM(plan, jnp.int32),
            pltpu.SemaphoreType.DMA((6,)),
            pltpu.SemaphoreType.DMA((len(SIDES),)),
            pltpu.SemaphoreType.DMA((len(SIDES),)),
        ]
        + [pltpu.SemaphoreType.DMA((devices,))] * 8
        + [pltpu.SemaphoreType.DMA((4,))],
        compiler_params=pltpu.CompilerParams(
            vmem_limit_bytes=44 * MIB, collective_id=0 if lean else 1, has_side_effects=True
        ),
        cost_estimate=pl.CostEstimate(flops=cells * 2000, bytes_accessed=density.size * 4, transcendentals=cells),
        name="exchange_lean" if lean else "exchange",
    )(density.reshape(height // RADIUS, RADIUS, width), known), spare


def place_kernel(cells, slots, arrived, volume, out, constraint, store_sem):
    devices, capacity = arrived.shape[:2]

    @pl.loop(0, devices)
    def _(d):
        for k in range(capacity):
            pltpu.make_async_copy(arrived.at[d, k], out.at[slots[d, k]], store_sem).start()

    mean = jnp.sum(volume[...], keepdims=True) / cells
    constraint[...] = mean / VOLUME_TARGET - 1.0
    landed = out.at[pl.ds(0, devices * capacity)]
    pltpu.make_async_copy(landed, landed, store_sem).wait()


def place(slots, arrived, volume, cells):
    count = arrived.shape[0] * arrived.shape[1]
    whole = pl.BlockSpec(memory_space=pltpu.VMEM)
    return pl.pallas_call(
        functools.partial(place_kernel, cells),
        out_shape=(
            jax.ShapeDtypeStruct((count, BS, BS), jnp.bfloat16),
            jax.ShapeDtypeStruct((1, 1), jnp.float32),
        ),
        in_specs=[pl.BlockSpec(memory_space=pltpu.SMEM), whole, whole],
        out_specs=(pl.BlockSpec(memory_space=pltpu.HBM), whole),
        scratch_shapes=[pltpu.SemaphoreType.DMA],
        compiler_params=pltpu.CompilerParams(vmem_limit_bytes=8 * MIB),
        cost_estimate=pl.CostEstimate(flops=0, bytes_accessed=2 * arrived.size * 2, transcendentals=0),
        name="place",
    )(slots, arrived, volume)


def per_device(density, design_mask, rebalance):
    sizes = (lax.axis_size("row"), lax.axis_size("col"))
    shape = design_mask.shape
    cells = float(density.size * sizes[0] * sizes[1])
    flat = design_mask.reshape(-1, BS)
    known = jnp.concatenate([rebalance.reshape(-1, BS), jnp.pad(flat, ((0, 8 - flat.shape[0]), (0, 0)))])

    def full():
        (arrived, volume, slots, _), _ = exchange(shape, density, known, sizes, False)
        return place(slots, arrived, volume, cells)

    if design_mask.size // (sizes[0] * sizes[1]) < 4:
        balanced, constraint = full()
        return balanced, constraint[0, 0]
    (arrived, volume, slots, most), spare = exchange(shape, density, known, sizes, True)
    balanced, constraint = lax.cond(most[0, 0] > spare, full, lambda: place(slots, arrived, volume, cells))
    return balanced, constraint[0, 0]


def solution(mesh):
    return jax.shard_map(
        per_device,
        mesh=mesh,
        in_specs=(P("row", "col"), P("row", "col"), P()),
        out_specs=(P(("row", "col"), None, None), P()),
        check_vma=False,
    )
```
